32 devices in a mesh: sub: 8 (over z, x), grp: 4 (over y, core).
Axes of the slice: x: 2, y: 2, z: 4, core: 2. Of those that a mesh axis runs over, the one named last changes fastest.
Arguments:
- solution: float32 [32, 128, 2048], P(('sub', 'grp')), may hold values from -6 to 6
- residual: float32 [32, 128, 2048], P(('sub', 'grp'))
- direction: float32 [32, 128, 2048], P(('sub', 'grp'))
- residual_product: float32 [128], replicated, may hold values from 65536 to 1310720
- neighbor_slots: int32 [32, 4], P(('sub', 'grp')), may hold values from 0 to 3, each once within a row
- coupling: bfloat16 [32, 96, 256, 128], P(('sub', 'grp')), may hold values from -0.375 to 0.375
- dirichlet_factor: bfloat16 [32, 96, 128, 128], P(('sub', 'grp')), may hold values from -0.5 to 0.5
- face_block: bfloat16 [32, 32, 128, 128], P(('sub', 'grp')), as said below
- neumann_factor: bfloat16 [32, 32, 128, 128], P(('sub', 'grp')), may hold values from -0.5 to 0.5
- primal_block: int32 [32, 128], P(('sub', 'grp')), may hold values from 0 to 31
- primal_basis: bfloat16 [32, 128, 128], P(('sub', 'grp')), may hold values from -1.5 to 1.5
- coarse_matrix: float32 [32, 9, 128, 128], P(('sub', 'grp')), may hold values from -0.17677669 to 0.17677669
- coarse_block_inverse: float32 [32, 128, 128], P(('sub', 'grp')), may hold values from -0.5 to 0.5
- coarse_pattern: int32 [32, 9], P(('sub', 'grp')), may hold values from 0 to 31, as said below
Outputs:
- new_solution: float32 [32, 128, 2048], P(('sub', 'grp'))
- new_residual: float32 [32, 128, 2048], P(('sub', 'grp'))
- new_direction: float32 [32, 128, 2048], P(('sub', 'grp'))
- new_product: float32 [128], replicated
The draws below stay inside these ranges and needn't reach their ends.
Inputs may be any that keep to these rules, and one draw needn't show every extreme that they name: `neighbor_slots`: each row orders the four local face slots: entry d is the slot of the face toward direction d (sub lower, sub upper, grp lower, grp upper). `coarse_pattern`: row t names 9 different subdomains, the first of them t itself; subdomain s lies on the device of index s along sub+grp, and every entry lies within 2 positions of row t along sub, cyclically. `face_block`: each block is symmetric with every eigenvalue at least 0.5.
All inputs are finite; a program needn't handle non-finite values.
Results may differ from the reference program's by a relative error of at most 0.0003.
Values sent between devices are 32-bit elements; how exact they have to be, the bound alone decides.
A program may use at most 128 MiB of HBM per device.

```python
import math
import jax
import jax.numpy as jnp
from jax import lax

LOAD_CASES = 128
FACE_SIZE = 1024
BLOCK_SIZE = 128
PRIMALS = 128
PATTERN_BLOCKS = 9
REACH_SUBS = 2
FACE_BLOCKS = 32
INNER_BLOCKS = 96
SUBDOMAINS = 32
N_SUB = 8
N_GRP = 4


def ramped_field(key, salt):
    full_shape = (SUBDOMAINS, LOAD_CASES, 2 * FACE_SIZE)
    base_key = jax.random.fold_in(key, salt)
    column = jnp.exp(jax.random.uniform(jax.random.fold_in(base_key, 1), (1, 1, 2 * FACE_SIZE), jnp.float32, math.log(0.3), math.log(3.0)))
    across = jnp.exp(jax.random.uniform(jax.random.fold_in(base_key, 2), (1, LOAD_CASES, 1), jnp.float32, math.log(0.6), math.log(2.0)))
    position = jnp.arange(SUBDOMAINS, dtype=jnp.float32) / (SUBDOMAINS - 1)
    values = jax.random.normal(jax.random.fold_in(base_key, 3), full_shape, jnp.float32)
    ramp_scale = jnp.exp(math.log(3.0) * position)
    return values * column * across * ramp_scale[:, None, None]


def draw_residual(key, part):
    return ramped_field(key, 11)


def draw_direction(key, part):
    return ramped_field(key, 23)


def draw_face_block(key, part):
    full_shape = (SUBDOMAINS, FACE_BLOCKS, BLOCK_SIZE, BLOCK_SIZE)
    mixing = jax.random.normal(jax.random.fold_in(key, 31), full_shape, jnp.float32)
    gram_part = jnp.einsum('sjab,sjcb->sjac', mixing, mixing) / BLOCK_SIZE
    low_end = 0.5
    high_end = 2.0
    diagonal = jnp.exp(jax.random.uniform(jax.random.fold_in(key, 32), full_shape[:3], jnp.float32, math.log(low_end), math.log(high_end)))
    return (gram_part + diagonal[..., None] * jnp.eye(BLOCK_SIZE, dtype=jnp.float32)).astype(jnp.bfloat16)


def draw_coarse_pattern(key, part):
    candidates = N_GRP * (2 * REACH_SUBS + 1) - 1
    row_ids = jnp.arange(SUBDOMAINS, dtype=jnp.int32)

    def one_row(row_id):
        shuffled = jax.random.permutation(jax.random.fold_in(jax.random.fold_in(key, 41), row_id), candidates)
        chosen = shuffled[:PATTERN_BLOCKS - 1].astype(jnp.int32)
        own_slot = REACH_SUBS * N_GRP + row_id % N_GRP
        chosen = chosen + (chosen >= own_slot).astype(jnp.int32)
        entry_sub = (row_id // N_GRP + chosen // N_GRP - REACH_SUBS) % N_SUB
        entries = entry_sub * N_GRP + chosen % N_GRP
        return jnp.concatenate([row_id[None], entries]).astype(jnp.int32)
    return jax.vmap(one_row)(row_ids)


def plant(values, key, least, largest):
    place = [jax.random.randint(jax.random.fold_in(key, axis), (), 0, length) for axis, length in enumerate(values.shape)]
    longest = values.shape.index(max(values.shape))
    beside = place[:longest] + [(place[longest] + 1) % values.shape[longest]] + place[longest + 1:]
    return values.at[tuple(place)].set(least).at[tuple(beside)].set(largest)


def level_of(rng, extent, pieces, least, largest):
    def one(dim, blocks):
        draws = jax.random.uniform(jax.random.fold_in(jax.random.fold_in(rng, 6), dim), (blocks,), jnp.float32, least / len(pieces), largest / len(pieces))
        return jnp.repeat(jnp.exp(draws), extent[dim] // blocks).reshape((-1,) + (1,) * (len(extent) - dim - 1))

    loudness = one(*pieces[0])
    for cut in pieces[1:]:
        loudness = loudness * one(*cut)
    return loudness


def noise(own_key, extent, width, bound, cuts=(), kind=jnp.bfloat16):
    values = jax.random.normal(own_key, extent, jnp.float32) * width
    if len(cuts) > 0:
        values = level_of(own_key, extent, cuts, -0.22, 0.18) * values
    return jnp.clip(values, min=-bound, max=bound).astype(kind)


def setup_inputs(seed: int = 0) -> dict:
    arg_keys = jax.random.split(jax.random.key(seed), 15)
    return {
        "solution": noise(arg_keys[0], (SUBDOMAINS, LOAD_CASES, 2 * FACE_SIZE), 1.0, 6.0, ((0, 32),), jnp.float32),
        "residual": draw_residual(jax.random.fold_in(arg_keys[14], 71), 0),
        "direction": draw_direction(jax.random.fold_in(arg_keys[14], 71), 0),
        "residual_product": jnp.clip(jnp.exp(jax.random.uniform(arg_keys[3], (LOAD_CASES,), jnp.float32, math.log(65536.0), math.log(1310720))), 65536.0, 1310720),
        "neighbor_slots": jax.vmap(lambda own: jax.random.permutation(own, 4))(jax.random.split(arg_keys[4], SUBDOMAINS)).reshape((SUBDOMAINS, 4)).astype(jnp.int32),
        "coupling": noise(arg_keys[5], (SUBDOMAINS, INNER_BLOCKS, 2 * BLOCK_SIZE, BLOCK_SIZE), (2 * BLOCK_SIZE) ** -0.5, 0.375, ((0, 32),)),
        "dirichlet_factor": noise(arg_keys[6], (SUBDOMAINS, INNER_BLOCKS, BLOCK_SIZE, BLOCK_SIZE), BLOCK_SIZE ** -0.5, 0.5, ((0, 32),)),
        "face_block": draw_face_block(jax.random.fold_in(arg_keys[14], 71), 0),
        "neumann_factor": noise(arg_keys[8], (SUBDOMAINS, FACE_BLOCKS, BLOCK_SIZE, BLOCK_SIZE), BLOCK_SIZE ** -0.5, 0.5, ((0, 32),)),
        "primal_block": plant(jax.random.randint(arg_keys[9], (SUBDOMAINS, PRIMALS), 0, FACE_BLOCKS), jax.random.fold_in(arg_keys[9], 1), 0, FACE_BLOCKS - 1).astype(jnp.int32),
        "primal_basis": noise(arg_keys[10], (SUBDOMAINS, PRIMALS, BLOCK_SIZE), (BLOCK_SIZE // 8) ** -0.5, 1.5, ((0, 32),)),
        "coarse_matrix": noise(arg_keys[11], (SUBDOMAINS, PATTERN_BLOCKS, PRIMALS, PRIMALS), (1.0 / (PATTERN_BLOCKS * PRIMALS) ** 0.5), 0.17677669, ((0, 32),), jnp.float32),
        "coarse_block_inverse": noise(arg_keys[12], (SUBDOMAINS, PRIMALS, PRIMALS), PRIMALS ** -0.5, 0.5, ((0, 32),), jnp.float32),
        "coarse_pattern": draw_coarse_pattern(jax.random.fold_in(arg_keys[14], 71), 0),
    }


highest_precision = lax.Precision.HIGHEST


def onehot_slots(neighbor_slots):
    return (neighbor_slots[:, :, None] == jnp.arange(4, dtype=jnp.int32)[None, None, :]).astype(jnp.float32)


def spread(owned_part, slot_onehot):
    face_width = owned_part.shape[2] // 2
    load_count = owned_part.shape[1]
    own_sub = owned_part[:, :, :face_width].reshape(N_SUB, N_GRP, load_count, face_width)
    own_grp = owned_part[:, :, face_width:].reshape(N_SUB, N_GRP, load_count, face_width)
    from_sub = jnp.roll(own_sub, 1, axis=0)
    from_grp = jnp.roll(own_grp, 1, axis=1)
    directed = jnp.stack([from_sub, own_sub, from_grp, own_grp], 2).reshape(SUBDOMAINS, 4, load_count, face_width)
    placed = jnp.einsum('sdk,sdlf->slkf', slot_onehot, directed, precision=highest_precision)
    return placed.reshape(SUBDOMAINS, load_count, FACE_BLOCKS, BLOCK_SIZE)


def collect(local_part, slot_onehot):
    load_count = local_part.shape[1]
    placed = local_part.reshape(SUBDOMAINS, load_count, 4, FACE_SIZE)
    directed = jnp.einsum('sdk,slkf->sdlf', slot_onehot, placed, precision=highest_precision)
    grid_form = directed.reshape(N_SUB, N_GRP, 4, load_count, FACE_SIZE)
    owned_sub = grid_form[:, :, 1] + jnp.roll(grid_form[:, :, 0], -1, axis=0)
    owned_grp = grid_form[:, :, 3] + jnp.roll(grid_form[:, :, 2], -1, axis=1)
    return jnp.concatenate([owned_sub, owned_grp], 3).reshape(SUBDOMAINS, load_count, 2 * FACE_SIZE)


def condensed(vector, couple, dirichlet, face_matrix):
    count_of_blocks = vector.shape[1]
    block_width = vector.shape[2]
    paired = jnp.concatenate([jnp.concatenate([vector, jnp.roll(vector, -(offset + 1), axis=1)], 2) for offset in range(3)], 1)
    interior = jnp.einsum('lib,ibk->lik', paired, couple, precision=highest_precision)
    middle = jnp.einsum('lik,ikm->lim', interior, dirichlet, precision=highest_precision)
    solved = jnp.einsum('lim,ikm->lik', middle, dirichlet, precision=highest_precision)
    returned = jnp.einsum('lik,ibk->lib', solved, couple, precision=highest_precision)
    result = jnp.einsum('ljb,jbk->ljk', vector, face_matrix, precision=highest_precision)
    for offset in range(3):
        portion = returned[:, offset * count_of_blocks:(offset + 1) * count_of_blocks]
        result = result + portion[:, :, :block_width] + jnp.roll(portion[:, :, block_width:], offset + 1, axis=1)
    return result


def apply_condensed(operands):
    vector, couple, dirichlet, face_matrix = operands
    return condensed(vector, couple.astype(jnp.float32), dirichlet.astype(jnp.float32), face_matrix.astype(jnp.float32))


def local_precondition(operands):
    halved, neumann, block_ids, basis = operands
    neumann = neumann.astype(jnp.float32)
    basis = basis.astype(jnp.float32)
    neumann_step = jnp.einsum('ljb,jbk->ljk', halved, neumann, precision=highest_precision)
    local_solve = jnp.einsum('ljk,jmk->ljm', neumann_step, neumann, precision=highest_precision)
    selector = (block_ids[:, None] == jnp.arange(halved.shape[1], dtype=jnp.int32)[None, :]).astype(jnp.float32)
    picked = jnp.einsum('ljb,cj->lcb', halved, selector, precision=highest_precision)
    coarse_residual = jnp.einsum('lcb,cb->lc', picked, basis, precision=highest_precision)
    return local_solve, coarse_residual


def spread_coarse(operands):
    coarse_correction, block_ids, basis = operands
    basis = basis.astype(jnp.float32)
    selector = (block_ids[:, None] == jnp.arange(FACE_BLOCKS, dtype=jnp.int32)[None, :]).astype(jnp.float32)
    weighted = coarse_correction[:, :, None] * basis[None]
    return jnp.einsum('lcb,cj->ljb', weighted, selector, precision=highest_precision)


def precondition(owned_part, slot_onehot, neumann_factor, primal_block, primal_basis, coarse_matrix, coarse_block_inverse, coarse_pattern):
    halved = spread(owned_part, slot_onehot) * 0.5
    local_solve, coarse_residual = lax.map(local_precondition, (halved, neumann_factor, primal_block, primal_basis))
    initial_step = jnp.einsum('pqe,pek->pqk', coarse_residual, coarse_block_inverse, precision=highest_precision)
    gathered = initial_step[coarse_pattern]
    adjacent_sum = jnp.einsum('skld,skde->sle', gathered, coarse_matrix, precision=highest_precision)
    coarse_correction = initial_step + jnp.einsum('iqc,icw->iqw', coarse_residual - adjacent_sum, coarse_block_inverse, precision=highest_precision)
    spread_back = lax.map(spread_coarse, (coarse_correction, primal_block, primal_basis))
    return collect(0.5 * (local_solve + spread_back), slot_onehot)


def reference(solution, residual, direction, residual_product, neighbor_slots, coupling, dirichlet_factor, face_block, neumann_factor, primal_block, primal_basis, coarse_matrix, coarse_block_inverse, coarse_pattern):
    slot_onehot = onehot_slots(neighbor_slots)
    local_image = lax.map(apply_condensed, (spread(direction, slot_onehot), coupling, dirichlet_factor, face_block))
    image = collect(local_image, slot_onehot)
    curvature = jnp.sum(direction * image, axis=(0, 2))
    step_length = residual_product / curvature
    new_solution = solution + step_length[None, :, None] * direction
    new_residual = residual - step_length[None, :, None] * image
    preconditioned = precondition(new_residual, slot_onehot, neumann_factor, primal_block, primal_basis, coarse_matrix, coarse_block_inverse, coarse_pattern)
    new_product = jnp.sum(new_residual * preconditioned, axis=(0, 2))
    step_ratio = new_product / residual_product
    new_direction = preconditioned + step_ratio[None, :, None] * direction
    return new_solution, new_residual, new_direction, new_product
```

```python
import functools

import jax
import jax.numpy as jnp
from jax import lax
from jax.experimental import pallas as pl
from jax.experimental.pallas import tpu as pltpu
from jax.sharding import PartitionSpec as P

REACH = 2
WINDOW = 2 * REACH + 1
MESH = pl.DeviceIdType.MESH
F32 = jnp.float32
BF16 = jnp.bfloat16
NN = (((1,), (0,)), ((), ()))
NT = (((1,), (1,)), ((), ()))


def split(value):
    high = value.astype(BF16)
    low = (value - high.astype(F32)).astype(BF16)
    return jnp.concatenate([high, low], 0)


def merge(value):
    half = value.shape[0] // 2
    return value[:half] + value[half:]


def dot(lhs, rhs, dims=NN):
    return lax.dot_general(lhs, rhs, dims, preferred_element_type=F32)


def exact(lhs, rhs):
    return lax.dot_general(
        lhs, rhs, NN, preferred_element_type=F32, precision=lax.Precision.HIGHEST
    )


def row_sums(value):
    return jnp.sum(value.T, axis=0, keepdims=True)


def as_columns(row, width):
    return jnp.broadcast_to(row, (width, row.shape[1])).T


def kernel(
    n_sub, n_grp,
    sol_h, res_h, dir_h, rp_ref, slots, coup_h, diri_h, face_h, neum_h, pb_ref, basis_h,
    cmat_h, cinv_h, pattern,
    osol_h, ores_h, odir_h, oprod,
    inv_s, U, R, Uhl, V, B, Y, RY, Hhl, H, LS, RLS, S, OD, Cw, Fd, Fb, Nf, basis, basisx,
    cmat, cinv, Wn, acc, cr2, RB, RP, SP, RC, corr, red_g, red_s, red_g2, red_s2, crs,
    stepb, csem, snd, rcv,
):
    ms = lax.axis_index("sub")
    mg = lax.axis_index("grp")
    width = basis.shape[0]
    nb = Fb.shape[0]
    fb = nb // 4
    n_q = Cw.shape[0] // nb
    counter = [0]
    pending = []

    def sub_at(offset):
        return (lax.rem(ms + offset + n_sub, n_sub), mg)

    def grp_at(offset):
        return (ms, lax.rem(mg + offset + n_grp, n_grp))

    def send(src, dst, device):
        i = counter[0]
        counter[0] += 1
        copy = pltpu.make_async_remote_copy(
            src_ref=src, dst_ref=dst, send_sem=snd.at[i], recv_sem=rcv.at[i],
            device_id=device, device_id_type=MESH,
        )
        copy.start()
        pending.append(copy)
        return copy

    def blocks(ref, d):
        return ref.at[pl.ds(d * fb, fb)]

    def columns(ref, half, k):
        return ref.at[0, :, pl.ds((half * fb + k) * width, width)]

    def fetch_face(hbm, half, buf, d, sem):
        for k in range(fb):
            pltpu.make_async_copy(columns(hbm, half, k), buf.at[d * fb + k], csem.at[sem]).start()

    def wait_face(buf, d, sem):
        pltpu.make_async_copy(blocks(buf, d), blocks(buf, d), csem.at[sem]).wait()

    def store_face(buf, d, hbm, half, sem):
        for k in range(fb):
            pltpu.make_async_copy(buf.at[d * fb + k], columns(hbm, half, k), csem.at[sem]).start()

    fetch_face(dir_h, 0, U, 1, 0)
    fetch_face(dir_h, 1, U, 3, 1)
    weight_copies = []
    for s in range(4):
        group = []
        for q in range(n_q):
            part = pl.ds(q * nb + s * fb, fb)
            group.append(pltpu.make_async_copy(coup_h.at[0, part], Cw.at[part], csem.at[10 + 7 * s + q]))
            group.append(pltpu.make_async_copy(diri_h.at[0, part], Fd.at[part], csem.at[10 + 7 * s + 3 + q]))
        part = pl.ds(s * fb, fb)
        group.append(pltpu.make_async_copy(face_h.at[0, part], Fb.at[part], csem.at[10 + 7 * s + 6]))
        weight_copies.append(group)

    barrier = pltpu.get_barrier_semaphore()
    for o in range(1, n_sub):
        pl.semaphore_signal(barrier, inc=1, device_id=sub_at(o), device_id_type=MESH)
    for o in range(1, n_grp):
        pl.semaphore_signal(barrier, inc=1, device_id=grp_at(o), device_id_type=MESH)
    for c in weight_copies[0]:
        c.start()
    fetch_face(res_h, 0, R, 1, 2)
    fetch_face(res_h, 1, R, 3, 3)
    small = [
        pltpu.make_async_copy(basis_h.at[0], basis, csem.at[4]),
        pltpu.make_async_copy(cmat_h.at[0], cmat, csem.at[5]),
        pltpu.make_async_copy(cinv_h.at[0], cinv, csem.at[6]),
        pltpu.make_async_copy(neum_h.at[0], Nf, csem.at[7]),
    ]
    small[0].start()
    for group in weight_copies[1:]:
        for c in group:
            c.start()
    for c in small[1:]:
        c.start()
    fetch_face(sol_h, 0, S, 0, 8)
    fetch_face(sol_h, 1, S, 1, 9)
    pl.semaphore_wait(barrier, n_sub + n_grp - 2)

    wait_face(U, 1, 0)
    u_sub = send(blocks(U, 1), blocks(U, 0), sub_at(1))
    wait_face(U, 3, 1)
    u_grp = send(blocks(U, 3), blocks(U, 2), grp_at(1))
    wait_face(R, 1, 2)
    r_sub = send(blocks(R, 1), blocks(R, 0), sub_at(1))
    wait_face(R, 3, 3)
    r_grp = send(blocks(R, 3), blocks(R, 2), grp_at(1))

    small[0].wait()
    basisx[...] = basis[...].astype(F32)
    primal = pb_ref[...].astype(F32)
    for side in range(2):
        SP[side] = primal - (slots[0, 2 * side] * fb).astype(F32)
    extra = []
    for side, device in ((0, sub_at(-1)), (1, grp_at(-1))):
        extra.append(send(basisx, RB.at[side], device))
        extra.append(send(SP.at[side], RP.at[side], device))

    for s in range(4):
        at = jnp.int32(0)
        for d in range(4):
            at = jnp.where(slots[0, d] == s, jnp.int32(d * fb), at)
        inv_s[s] = at
    acc[...] = jnp.zeros_like(acc)

    u_grp.wait_recv()
    u_sub.wait_recv()

    for s in range(4):
        def prepare(k, carry, s=s):
            Uhl[s * fb + k] = split(U[inv_s[s] + k])
            return carry
        lax.fori_loop(0, fb, prepare, 0, unroll=2)

    for s in range(4):
        for c in weight_copies[s]:
            c.wait()

        def interior(k, carry, s=s):
            j = s * fb + k
            uj = Uhl[j]
            v = merge(dot(uj, Fb[j]))
            V[j] = v
            total = U[inv_s[s] + k] * v
            for q in range(n_q):
                m = lax.rem(j + q + 1, nb)
                n = q * nb + j
                a = merge(dot(jnp.concatenate([uj, Uhl[m]], 1), Cw[n]))
                t = merge(dot(split(a), Fd[n]))
                total = total + t * t
                B[n] = split(merge(dot(split(t), Fd[n], NT)))
            acc[...] += total
            return carry
        lax.fori_loop(0, fb, interior, 0, unroll=2)

    def reduce_start(row, red, first, index, count, at):
        red[index] = row
        return [send(red.at[index], red.at[index], at(o)) for o in range(1, count)]

    def reduce_end(copies, red, count):
        for c in copies:
            c.wait_recv()
        for c in copies:
            c.wait_send()
            pending[:] = [other for other in pending if other is not c]
        total = red[0]
        for i in range(1, count):
            total = total + red[i]
        return total

    copies = reduce_start(row_sums(acc[...]), red_g, True, mg, n_grp, grp_at)

    def returned(d):
        def body(k, carry):
            j = slots[0, d] * fb + k
            lhs = []
            rhs = []
            for q in range(n_q):
                n = q * nb + j
                p = q * nb + lax.rem(j - q - 1 + nb, nb)
                lhs += [B[n], B[p]]
                rhs += [Cw[n, :width], Cw[p, width:]]
            y = merge(dot(jnp.concatenate(lhs, 1), jnp.concatenate(rhs, 1), NT))
            Y[d * fb + k] = y + V[j]
            return carry
        lax.fori_loop(0, fb, body, 0, unroll=2)

    returned(0)
    part = reduce_end(copies, red_g, n_grp)
    copies = reduce_start(part, red_s, True, ms, n_sub, sub_at)
    ys = {}
    ys[1] = send(blocks(Y, 0), blocks(RY, 1), sub_at(-1))
    returned(1)
    ys[0] = send(blocks(Y, 1), blocks(RY, 0), sub_at(1))
    returned(2)
    ys[3] = send(blocks(Y, 2), blocks(RY, 3), grp_at(-1))
    returned(3)
    ys[2] = send(blocks(Y, 3), blocks(RY, 2), grp_at(1))
    curvature = reduce_end(copies, red_s, n_sub)
    rp = rp_ref[...]
    stepb[...] = as_columns(rp / curvature, width)

    wait_face(S, 0, 8)
    wait_face(S, 1, 9)
    for half in range(2):
        def iterate(k, carry, half=half):
            S[half * fb + k] = S[half * fb + k] + stepb[...] * U[(2 * half + 1) * fb + k]
            return carry
        lax.fori_loop(0, fb, iterate, 0, unroll=2)
        store_face(S, half, osol_h, half, 8 + half)

    for c in extra:
        c.wait_recv()
    r_grp.wait_recv()
    r_sub.wait_recv()
    for c in small[1:]:
        c.wait()
    pbc = as_columns(primal, width)
    cr2[...] = jnp.zeros_like(cr2)
    acc[...] = jnp.zeros_like(acc)
    basis32 = basisx[...]

    def pick(j):
        return jnp.where(pbc == j.astype(F32), basis32, 0.0).astype(BF16)

    def residual_face(d):
        ys[d].wait_recv()

        def body(k, carry):
            i = d * fb + k
            new = R[i] - stepb[...] * (Y[i] + RY[i])
            H[i] = new
            hl = split(new * 0.5)
            Hhl[i] = hl
            cr2[...] += dot(hl, pick(slots[0, d] * fb + k), NT)
            return carry
        lax.fori_loop(0, fb, body, 0, unroll=2)
        if d % 2 == 1:
            store_face(H, d, ores_h, d // 2, d - 1 - d // 2)

    def local_face(d):
        def body(k, carry):
            i = d * fb + k
            factor = Nf[slots[0, d] * fb + k]
            t = merge(dot(Hhl[i], factor))
            acc[...] += t * t
            LS[i] = 0.5 * merge(dot(split(t), factor, NT))
            return carry
        lax.fori_loop(0, fb, body, 0, unroll=2)

    residual_face(2)
    local_face(2)
    ls_grp = send(blocks(LS, 2), blocks(RLS, 1), grp_at(-1))
    residual_face(3)
    local_face(3)
    residual_face(1)
    residual_face(0)
    cr = merge(cr2[...])
    crs[...] = cr
    first = exact(cr, cinv[...])

    def place(g, p):
        return Wn.at[g * WINDOW + p]

    Wn[mg * WINDOW + REACH] = first
    arrivals = {}
    for o in (1, -1, 2, -2):
        p = REACH - o
        arrivals[p] = send(place(mg, REACH), place(mg, p), sub_at(o))
    order = (REACH, REACH - 2, REACH + 2, REACH - 1, REACH + 1)
    if n_grp == 4:
        near = (ms, mg + 1 - 2 * lax.rem(mg, 2))
        far = lax.rem(mg + 2, 4)
        far_copies = {}
        column_copies = []

        def pass_on(p):
            far_copies[p] = send(place(mg, p), place(mg, p), (ms, far))
            column_copies.append(send(place(mg, p), place(mg, p), near))
        pass_on(REACH)
        local_face(0)
        ls_sub = send(blocks(LS, 0), blocks(RLS, 0), sub_at(-1))
        for p in order[1:]:
            arrivals[p].wait_recv()
            pass_on(p)
        local_face(1)
        for p in order:
            far_copies[p].wait_recv()
            column_copies.append(send(place(far, p), place(far, p), near))
        for c in column_copies:
            c.wait_recv()
    else:
        column_copies = []
        local_face(0)
        ls_sub = send(blocks(LS, 0), blocks(RLS, 0), sub_at(-1))
        for p in order:
            if p != REACH:
                arrivals[p].wait_recv()
            for o in range(1, n_grp):
                column_copies.append(send(place(mg, p), place(mg, p), grp_at(o)))
        local_face(1)
        for c in column_copies:
            c.wait_recv()

    chosen = []
    for k in range(cmat.shape[0]):
        entry = pattern[0, k]
        p = lax.min(lax.rem(entry // n_grp - ms + REACH + n_sub, n_sub), jnp.int32(WINDOW - 1))
        chosen.append(Wn[lax.rem(entry, n_grp) * WINDOW + p])
    adjacent = exact(
        jnp.concatenate(chosen, 1), cmat[...].reshape(cmat.shape[0] * width, width)
    )
    correction = Wn[mg * WINDOW + REACH] + exact(crs[...] - adjacent, cinv[...])
    corr[...] = correction
    c_sub = send(corr, RC.at[0], sub_at(-1))
    c_grp = send(corr, RC.at[1], grp_at(-1))
    product_row = row_sums(acc[...] + correction * crs[...])
    copies = reduce_start(product_row, red_g2, False, mg, n_grp, grp_at)

    corr_hl = split(correction * 0.5)

    def own_spread(d):
        def body(k, carry):
            i = d * fb + k
            LS[i] = LS[i] + merge(dot(corr_hl, pick(slots[0, d] * fb + k)))
            return carry
        lax.fori_loop(0, fb, body, 0, unroll=2)

    own_spread(1)
    part = reduce_end(copies, red_g2, n_grp)
    copies = reduce_start(part, red_s2, False, ms, n_sub, sub_at)
    own_spread(3)

    def borrowed_spread(side):
        d = 2 * side + 1
        relative = as_columns(RP[side], width)
        other = RB[side]
        other_hl = split(RC[side] * 0.5)

        def body(k, carry):
            i = d * fb + k
            rows = jnp.where(relative == k.astype(F32), other, 0.0).astype(BF16)
            OD[side * fb + k] = LS[i] + RLS[side * fb + k] + merge(dot(other_hl, rows))
            return carry
        lax.fori_loop(0, fb, body, 0, unroll=2)

    ls_grp.wait_recv()
    c_grp.wait_recv()
    borrowed_spread(1)
    ls_sub.wait_recv()
    c_sub.wait_recv()
    borrowed_spread(0)
    product = reduce_end(copies, red_s2, n_sub)
    oprod[...] = product
    ratio = as_columns(product / rp, width)
    for half in range(2):
        def advance(k, carry, half=half):
            OD[half * fb + k] = OD[half * fb + k] + ratio * U[(2 * half + 1) * fb + k]
            return carry
        lax.fori_loop(0, fb, advance, 0, unroll=2)
        store_face(OD, half, odir_h, half, 2 + half)

    for half in range(2):
        wait_face(S, half, 8 + half)
        wait_face(H, 2 * half + 1, half)
        wait_face(OD, half, 2 + half)
    for c in pending:
        c.wait_send()


def shards(
    solution, residual, direction, residual_product, neighbor_slots, coupling,
    dirichlet_factor, face_block, neumann_factor, primal_block, primal_basis,
    coarse_matrix, coarse_block_inverse, coarse_pattern,
):
    n_sub = lax.axis_size("sub")
    n_grp = lax.axis_size("grp")
    loads = direction.shape[1]
    nb = face_block.shape[1]
    width = face_block.shape[2]
    fb = nb // 4
    inner = coupling.shape[1]
    copies = 8 + 4 + 2 + 2 + 4 + 3 * WINDOW + 2 * (n_sub + n_grp) + WINDOW * n_grp
    hbm = pl.BlockSpec(memory_space=pl.ANY)
    vmem = pl.BlockSpec(memory_space=pltpu.VMEM)
    smem = pl.BlockSpec(memory_space=pltpu.SMEM)

    def block(count, dtype=F32, rows=loads):
        return pltpu.VMEM((count, rows, width), dtype)

    scratch = [
        pltpu.SMEM((4,), jnp.int32),
        block(nb), block(nb), block(nb, BF16, 2 * loads), block(nb),
        block(inner, BF16, 2 * loads), block(nb), block(nb),
        block(nb, BF16, 2 * loads), block(nb), block(nb), block(2 * fb), block(2 * fb),
        block(2 * fb),
        pltpu.VMEM(coupling.shape[1:], BF16), pltpu.VMEM(dirichlet_factor.shape[1:], BF16),
        pltpu.VMEM(face_block.shape[1:], BF16), pltpu.VMEM(neumann_factor.shape[1:], BF16),
        pltpu.VMEM(primal_basis.shape[1:], BF16), pltpu.VMEM(primal_basis.shape[1:], F32),
        pltpu.VMEM(coarse_matrix.shape[1:], F32), pltpu.VMEM(coarse_block_inverse.shape[1:], F32),
        block(n_grp * WINDOW),
        pltpu.VMEM((loads, width), F32),
        pltpu.VMEM((2 * loads, width), F32),
        block(2), pltpu.VMEM((2, 1, width), F32), pltpu.VMEM((2, 1, width), F32),
        block(2), pltpu.VMEM((loads, width), F32),
        pltpu.VMEM((n_grp, 1, loads), F32), pltpu.VMEM((n_sub, 1, loads), F32),
        pltpu.VMEM((n_grp, 1, loads), F32), pltpu.VMEM((n_sub, 1, loads), F32),
        pltpu.VMEM((loads, width), F32), pltpu.VMEM((loads, width), F32),
        pltpu.SemaphoreType.DMA((40,)),
        pltpu.SemaphoreType.DMA((copies,)), pltpu.SemaphoreType.DMA((copies,)),
    ]
    field = jax.ShapeDtypeStruct(solution.shape, F32)
    outs = pl.pallas_call(
        functools.partial(kernel, n_sub, n_grp),
        out_shape=(field, field, field, jax.ShapeDtypeStruct((1, loads), F32)),
        in_specs=[hbm, hbm, hbm, vmem, smem, hbm, hbm, hbm, hbm, vmem, hbm, hbm, hbm, smem],
        out_specs=(hbm, hbm, hbm, vmem),
        scratch_shapes=scratch,
        compiler_params=pltpu.CompilerParams(
            collective_id=0, has_side_effects=True, vmem_limit_bytes=58 * 1024 * 1024
        ),
    )(
        solution, residual, direction, residual_product.reshape(1, -1), neighbor_slots,
        coupling, dirichlet_factor, face_block, neumann_factor, primal_block, primal_basis,
        coarse_matrix, coarse_block_inverse, coarse_pattern,
    )
    return outs[0], outs[1], outs[2], outs[3].reshape(-1)


def solution(mesh):
    rows = P(("sub", "grp"))
    in_specs = (rows, rows, rows, P()) + (rows,) * 10
    out_specs = (rows, rows, rows, P())
    return jax.shard_map(shards, mesh=mesh, in_specs=in_specs, out_specs=out_specs, check_vma=False)
```

```python
import functools

import jax
import jax.numpy as jnp
from jax import lax
from jax.experimental import pallas as pl
from jax.experimental.pallas import tpu as pltpu
from jax.sharding import PartitionSpec as P

REACH = 2
WINDOW = 2 * REACH + 1
MESH = pl.DeviceIdType.MESH
F32 = jnp.float32
BF16 = jnp.bfloat16
NN = (((1,), (0,)), ((), ()))
NT = (((1,), (1,)), ((), ()))


def split(value):
    high = value.astype(BF16)
    low = (value - high.astype(F32)).astype(BF16)
    return jnp.concatenate([high, low], 0)


def merge(value):
    half = value.shape[0] // 2
    return value[:half] + value[half:]


def dot(lhs, rhs, dims=NN):
    return lax.dot_general(lhs, rhs, dims, preferred_element_type=F32)


def exact(lhs, rhs):
    return lax.dot_general(
        lhs, rhs, NN, preferred_element_type=F32, precision=lax.Precision.HIGHEST
    )


def row_sums(value):
    return jnp.sum(value.T, axis=0, keepdims=True)


def as_columns(row, width):
    return jnp.broadcast_to(row, (width, row.shape[1])).T


def kernel(
    n_sub, n_grp,
    sol_h, res_h, dir_h, rp_ref, slots, coup_h, diri_h, face_h, neum_h, pb_ref, basis_h,
    cmat_h, cinv_h, pattern,
    osol_h, ores_h, odir_h, oprod,
    inv_s, U, R, Uhl, V, B, Y, RY, Hhl, H, LS, NXs, NXr, S, OD, Cw, Fd, Fb, Nf, basis, basisx,
    cmat, cinv, Wn, acc, cr2, crn2, crn, rcr, rel, RB, RP, SP, RC, corr, red_g, red_s, red_g2, red_s2, crs,
    stepb, csem, snd, rcv,
):
    ms = lax.axis_index("sub")
    mg = lax.axis_index("grp")
    width = basis.shape[0]
    nb = Fb.shape[0]
    fb = nb // 4
    n_q = Cw.shape[0] // nb
    counter = [0]
    pending = []

    def sub_at(offset):
        return (lax.rem(ms + offset + n_sub, n_sub), mg)

    def grp_at(offset):
        return (ms, lax.rem(mg + offset + n_grp, n_grp))

    def send(src, dst, device):
        i = counter[0]
        counter[0] += 1
        copy = pltpu.make_async_remote_copy(
            src_ref=src, dst_ref=dst, send_sem=snd.at[i], recv_sem=rcv.at[i],
            device_id=device, device_id_type=MESH,
        )
        copy.start()
        pending.append(copy)
        return copy

    def blocks(ref, d):
        return ref.at[pl.ds(d * fb, fb)]

    def columns(ref, half, k):
        return ref.at[0, :, pl.ds((half * fb + k) * width, width)]

    def fetch_face(hbm, half, buf, d, sem):
        for k in range(fb):
            pltpu.make_async_copy(columns(hbm, half, k), buf.at[d * fb + k], csem.at[sem]).start()

    def wait_face(buf, d, sem):
        pltpu.make_async_copy(blocks(buf, d), blocks(buf, d), csem.at[sem]).wait()

    def store_face(buf, d, hbm, half, sem):
        for k in range(fb):
            pltpu.make_async_copy(buf.at[d * fb + k], columns(hbm, half, k), csem.at[sem]).start()

    fetch_face(dir_h, 0, U, 1, 0)
    fetch_face(dir_h, 1, U, 3, 1)
    weight_copies = []
    for s in range(4):
        group = []
        for q in range(n_q):
            part = pl.ds(q * nb + s * fb, fb)
            group.append(pltpu.make_async_copy(coup_h.at[0, part], Cw.at[part], csem.at[10 + 7 * s + q]))
            group.append(pltpu.make_async_copy(diri_h.at[0, part], Fd.at[part], csem.at[10 + 7 * s + 3 + q]))
        part = pl.ds(s * fb, fb)
        group.append(pltpu.make_async_copy(face_h.at[0, part], Fb.at[part], csem.at[10 + 7 * s + 6]))
        weight_copies.append(group)

    barrier = pltpu.get_barrier_semaphore()
    for o in range(1, n_sub):
        pl.semaphore_signal(barrier, inc=1, device_id=sub_at(o), device_id_type=MESH)
    for o in range(1, n_grp):
        pl.semaphore_signal(barrier, inc=1, device_id=grp_at(o), device_id_type=MESH)
    for c in weight_copies[0]:
        c.start()
    fetch_face(res_h, 0, R, 1, 2)
    fetch_face(res_h, 1, R, 3, 3)
    small = [
        pltpu.make_async_copy(basis_h.at[0], basis, csem.at[4]),
        pltpu.make_async_copy(cmat_h.at[0], cmat, csem.at[5]),
        pltpu.make_async_copy(cinv_h.at[0], cinv, csem.at[6]),
        pltpu.make_async_copy(neum_h.at[0], Nf, csem.at[7]),
    ]
    small[0].start()
    small[3].start()
    for group in weight_copies[1:]:
        for c in group:
            c.start()
    for c in small[1:3]:
        c.start()
    fetch_face(sol_h, 0, S, 0, 8)
    fetch_face(sol_h, 1, S, 1, 9)
    pl.semaphore_wait(barrier, n_sub + n_grp - 2)

    wait_face(U, 1, 0)
    u_sub = send(blocks(U, 1), blocks(U, 0), sub_at(1))
    wait_face(U, 3, 1)
    u_grp = send(blocks(U, 3), blocks(U, 2), grp_at(1))
    small[3].wait()
    for side in range(2):
        def widen(k, carry, side=side):
            NXs[side * fb + k] = Nf[slots[0, 2 * side] * fb + k].astype(F32)
            return carry
        lax.fori_loop(0, fb, widen, 0, unroll=2)

    small[0].wait()
    basisx[...] = basis[...].astype(F32)
    primal = pb_ref[...].astype(F32)
    for side in range(2):
        SP[side] = primal - (slots[0, 2 * side] * fb).astype(F32)
    for s in range(4):
        at = jnp.int32(0)
        for d in range(4):
            at = jnp.where(slots[0, d] == s, jnp.int32(d * fb), at)
        inv_s[s] = at
    acc[...] = jnp.zeros_like(acc)

    u_grp.wait_recv()
    u_sub.wait_recv()
    extra = []
    for side, device in ((0, sub_at(-1)), (1, grp_at(-1))):
        extra.append(send(blocks(NXs, side), blocks(NXr, side), device))
        extra.append(send(basisx, RB.at[side], device))
        extra.append(send(SP.at[side], RP.at[side], device))

    for s in range(4):
        def prepare(k, carry, s=s):
            Uhl[s * fb + k] = split(U[inv_s[s] + k])
            return carry
        lax.fori_loop(0, fb, prepare, 0, unroll=2)

    for s in range(4):
        for c in weight_copies[s]:
            c.wait()

        def interior(k, carry, s=s):
            j = s * fb + k
            uj = Uhl[j]
            v = merge(dot(uj, Fb[j]))
            V[j] = v
            total = U[inv_s[s] + k] * v
            for q in range(n_q):
                m = lax.rem(j + q + 1, nb)
                n = q * nb + j
                a = merge(dot(jnp.concatenate([uj, Uhl[m]], 1), Cw[n]))
                t = merge(dot(split(a), Fd[n]))
                total = total + t * t
                B[n] = split(merge(dot(split(t), Fd[n], NT)))
            acc[...] += total
            return carry
        lax.fori_loop(0, fb, interior, 0, unroll=2)

    def reduce_start(row, red, first, index, count, at):
        red[index] = row
        return [send(red.at[index], red.at[index], at(o)) for o in range(1, count)]

    def reduce_end(copies, red, count):
        for c in copies:
            c.wait_recv()
        for c in copies:
            c.wait_send()
            pending[:] = [other for other in pending if other is not c]
        total = red[0]
        for i in range(1, count):
            total = total + red[i]
        return total

    copies = reduce_start(row_sums(acc[...]), red_g, True, mg, n_grp, grp_at)

    def returned(d):
        def body(k, carry):
            j = slots[0, d] * fb + k
            lhs = []
            rhs = []
            for q in range(n_q):
                n = q * nb + j
                p = q * nb + lax.rem(j - q - 1 + nb, nb)
                lhs += [B[n], B[p]]
                rhs += [Cw[n, :width], Cw[p, width:]]
            y = merge(dot(jnp.concatenate(lhs, 1), jnp.concatenate(rhs, 1), NT))
            Y[d * fb + k] = y + V[j]
            return carry
        lax.fori_loop(0, fb, body, 0, unroll=2)

    returned(0)
    part = reduce_end(copies, red_g, n_grp)
    copies = reduce_start(part, red_s, True, ms, n_sub, sub_at)
    ys = {}
    ys[1] = send(blocks(Y, 0), blocks(RY, 1), sub_at(-1))
    returned(2)
    ys[3] = send(blocks(Y, 2), blocks(RY, 3), grp_at(-1))
    returned(1)
    returned(3)
    curvature = reduce_end(copies, red_s, n_sub)
    rp = rp_ref[...]
    stepb[...] = as_columns(rp / curvature, width)

    wait_face(S, 0, 8)
    wait_face(S, 1, 9)
    for half in range(2):
        def iterate(k, carry, half=half):
            S[half * fb + k] = S[half * fb + k] + stepb[...] * U[(2 * half + 1) * fb + k]
            return carry
        lax.fori_loop(0, fb, iterate, 0, unroll=2)
        store_face(S, half, osol_h, half, 8 + half)

    for c in extra:
        c.wait_recv()
    for c in small[1:3]:
        c.wait()
    wait_face(R, 1, 2)
    wait_face(R, 3, 3)
    for side in range(2):
        rel[side] = as_columns(RP[side], width)
    pbc = as_columns(primal, width)
    cr2[...] = jnp.zeros_like(cr2)
    acc[...] = jnp.zeros_like(acc)
    basis32 = basisx[...]

    def pick(j):
        return jnp.where(pbc == j.astype(F32), basis32, 0.0).astype(BF16)

    def pick_other(side, k):
        return jnp.where(rel[side] == k.astype(F32), RB[side], 0.0).astype(BF16)

    def residual_face(d):
        side = d // 2
        ys[d].wait_recv()
        crn2[...] = jnp.zeros_like(crn2)

        def body(k, carry):
            i = d * fb + k
            new = R[i] - stepb[...] * (Y[i] + RY[i])
            H[i] = new
            hl = split(new * 0.5)
            Hhl[i] = hl
            cr2[...] += dot(hl, pick(slots[0, d] * fb + k), NT)
            crn2[...] += dot(hl, pick_other(side, k), NT)
            return carry
        lax.fori_loop(0, fb, body, 0, unroll=2)
        crn[side] = merge(crn2[...])
        store_face(H, d, ores_h, side, side)

    def local_face(d):
        side = d // 2

        def body(k, carry):
            i = d * fb + k
            hl = Hhl[i]
            factor = Nf[slots[0, d] * fb + k]
            other = NXr[side * fb + k].astype(BF16)
            t = merge(dot(hl, factor))
            w = merge(dot(hl, other))
            acc[...] += t * t + w * w
            LS[i] = 0.5 * (merge(dot(split(t), factor, NT)) + merge(dot(split(w), other, NT)))
            return carry
        lax.fori_loop(0, fb, body, 0, unroll=2)

    residual_face(3)
    cr_grp = send(crn.at[1], rcr.at[1], grp_at(1))
    residual_face(1)
    cr_sub = send(crn.at[0], rcr.at[0], sub_at(1))
    local_face(3)
    cr_grp.wait_recv()
    cr_sub.wait_recv()
    cr = merge(cr2[...]) + rcr[0] + rcr[1]
    crs[...] = cr
    first = exact(cr, cinv[...])

    def place(g, p):
        return Wn.at[g * WINDOW + p]

    Wn[mg * WINDOW + REACH] = first
    arrivals = {}
    for o in (1, -1, 2, -2):
        p = REACH - o
        arrivals[p] = send(place(mg, REACH), place(mg, p), sub_at(o))
    order = (REACH, REACH - 2, REACH + 2, REACH - 1, REACH + 1)
    if n_grp == 4:
        near = (ms, mg + 1 - 2 * lax.rem(mg, 2))
        far = lax.rem(mg + 2, 4)
        far_copies = {}
        column_copies = []

        def pass_on(p):
            far_copies[p] = send(place(mg, p), place(mg, p), (ms, far))
            column_copies.append(send(place(mg, p), place(mg, p), near))
        pass_on(REACH)
        local_face(1)
        for p in order[1:]:
            arrivals[p].wait_recv()
            pass_on(p)
        for p in order:
            far_copies[p].wait_recv()
            column_copies.append(send(place(far, p), place(far, p), near))
        for c in column_copies:
            c.wait_recv()
    else:
        column_copies = []
        local_face(1)
        for p in order:
            if p != REACH:
                arrivals[p].wait_recv()
            for o in range(1, n_grp):
                column_copies.append(send(place(mg, p), place(mg, p), grp_at(o)))
        for c in column_copies:
            c.wait_recv()

    chosen = []
    for k in range(cmat.shape[0]):
        entry = pattern[0, k]
        p = lax.min(lax.rem(entry // n_grp - ms + REACH + n_sub, n_sub), jnp.int32(WINDOW - 1))
        chosen.append(Wn[lax.rem(entry, n_grp) * WINDOW + p])
    adjacent = exact(
        jnp.concatenate(chosen, 1), cmat[...].reshape(cmat.shape[0] * width, width)
    )
    correction = Wn[mg * WINDOW + REACH] + exact(crs[...] - adjacent, cinv[...])
    corr[...] = correction
    c_sub = send(corr, RC.at[0], sub_at(-1))
    c_grp = send(corr, RC.at[1], grp_at(-1))
    product_row = row_sums(acc[...] + correction * crs[...])
    copies = reduce_start(product_row, red_g2, False, mg, n_grp, grp_at)

    corr_hl = split(correction * 0.5)

    def own_spread(d):
        def body(k, carry):
            i = d * fb + k
            LS[i] = LS[i] + merge(dot(corr_hl, pick(slots[0, d] * fb + k)))
            return carry
        lax.fori_loop(0, fb, body, 0, unroll=2)

    own_spread(1)
    part = reduce_end(copies, red_g2, n_grp)
    copies = reduce_start(part, red_s2, False, ms, n_sub, sub_at)
    own_spread(3)

    def borrowed_spread(side):
        d = 2 * side + 1
        other_hl = split(RC[side] * 0.5)

        def body(k, carry):
            i = d * fb + k
            rows = pick_other(side, k)
            OD[side * fb + k] = LS[i] + merge(dot(other_hl, rows))
            return carry
        lax.fori_loop(0, fb, body, 0, unroll=2)

    c_grp.wait_recv()
    borrowed_spread(1)
    c_sub.wait_recv()
    borrowed_spread(0)
    product = reduce_end(copies, red_s2, n_sub)
    oprod[...] = product
    ratio = as_columns(product / rp, width)
    for half in range(2):
        def advance(k, carry, half=half):
            OD[half * fb + k] = OD[half * fb + k] + ratio * U[(2 * half + 1) * fb + k]
            return carry
        lax.fori_loop(0, fb, advance, 0, unroll=2)
        store_face(OD, half, odir_h, half, 2 + half)

    for half in range(2):
        wait_face(S, half, 8 + half)
        wait_face(H, 2 * half + 1, half)
        wait_face(OD, half, 2 + half)
    for c in pending:
        c.wait_send()


def shards(
    solution, residual, direction, residual_product, neighbor_slots, coupling,
    dirichlet_factor, face_block, neumann_factor, primal_block, primal_basis,
    coarse_matrix, coarse_block_inverse, coarse_pattern,
):
    n_sub = lax.axis_size("sub")
    n_grp = lax.axis_size("grp")
    loads = direction.shape[1]
    nb = face_block.shape[1]
    width = face_block.shape[2]
    fb = nb // 4
    inner = coupling.shape[1]
    copies = 8 + 4 + 2 + 2 + 4 + 3 * WINDOW + 2 * (n_sub + n_grp) + WINDOW * n_grp
    hbm = pl.BlockSpec(memory_space=pltpu.HBM)
    free = pl.BlockSpec(memory_space=pl.ANY)
    vmem = pl.BlockSpec(memory_space=pltpu.VMEM)
    smem = pl.BlockSpec(memory_space=pltpu.SMEM)

    def block(count, dtype=F32, rows=loads):
        return pltpu.VMEM((count, rows, width), dtype)

    scratch = [
        pltpu.SMEM((4,), jnp.int32),
        block(nb), block(nb), block(nb, BF16, 2 * loads), block(nb),
        block(inner, BF16, 2 * loads), block(nb), block(nb),
        block(nb, BF16, 2 * loads), block(nb), block(nb), block(2 * fb), block(2 * fb),
        block(2 * fb), block(2 * fb),
        pltpu.VMEM(coupling.shape[1:], BF16), pltpu.VMEM(dirichlet_factor.shape[1:], BF16),
        pltpu.VMEM(face_block.shape[1:], BF16), pltpu.VMEM(neumann_factor.shape[1:], BF16),
        pltpu.VMEM(primal_basis.shape[1:], BF16), pltpu.VMEM(primal_basis.shape[1:], F32),
        pltpu.VMEM(coarse_matrix.shape[1:], F32), pltpu.VMEM(coarse_block_inverse.shape[1:], F32),
        block(n_grp * WINDOW),
        pltpu.VMEM((loads, width), F32),
        pltpu.VMEM((2 * loads, width), F32), pltpu.VMEM((2 * loads, width), F32),
        block(2), block(2), block(2), block(2), pltpu.VMEM((2, 1, width), F32), pltpu.VMEM((2, 1, width), F32),
        block(2), pltpu.VMEM((loads, width), F32),
        pltpu.VMEM((n_grp, 1, loads), F32), pltpu.VMEM((n_sub, 1, loads), F32),
        pltpu.VMEM((n_grp, 1, loads), F32), pltpu.VMEM((n_sub, 1, loads), F32),
        pltpu.VMEM((loads, width), F32), pltpu.VMEM((loads, width), F32),
        pltpu.SemaphoreType.DMA((40,)),
        pltpu.SemaphoreType.DMA((copies,)), pltpu.SemaphoreType.DMA((copies,)),
    ]
    field = jax.ShapeDtypeStruct(solution.shape, F32)
    outs = pl.pallas_call(
        functools.partial(kernel, n_sub, n_grp),
        out_shape=(field, field, field, jax.ShapeDtypeStruct((1, loads), F32)),
        in_specs=[hbm, hbm, hbm, vmem, smem, hbm, hbm, hbm, hbm, vmem, hbm, hbm, hbm, smem],
        out_specs=(free, free, free, vmem),
        scratch_shapes=scratch,
        compiler_params=pltpu.CompilerParams(
            collective_id=0, has_side_effects=True, vmem_limit_bytes=62 * 1024 * 1024
        ),
    )(
        solution, residual, direction, residual_product.reshape(1, -1), neighbor_slots,
        coupling, dirichlet_factor, face_block, neumann_factor, primal_block, primal_basis,
        coarse_matrix, coarse_block_inverse, coarse_pattern,
    )
    return outs[0], outs[1], outs[2], outs[3].reshape(-1)


def solution(mesh):
    rows = P(("sub", "grp"))
    in_specs = (rows, rows, rows, P()) + (rows,) * 10
    out_specs = (rows, rows, rows, P())
    return jax.shard_map(shards, mesh=mesh, in_specs=in_specs, out_specs=out_specs, check_vma=False)
```
